32 devices in a mesh: band: 8 (over z, y), grid: 4 (over x, core).
Axes of the slice: x: 2, y: 2, z: 4, core: 2. Of those that a mesh axis runs over, the one named last changes fastest.
Arguments:
- orbitals: bfloat16 [8, 128, 128, 128], P('band', 'grid'), may hold values from -3 to 3
- trial_vectors: bfloat16 [2, 8, 128, 128, 128], P(None, 'band', 'grid'), may hold values from -6 to 6
- alda_kernel: float32 [128, 128, 128], P('grid'), may hold values from -2 to -0.5
- local_potential: float32 [128, 128, 128], P('grid'), may hold values from -2 to 1
- band_energies: float32 [8], P('band'), may hold values from -1.5 to -0.2
Outputs:
- sigma_real: float32 [2, 8, 128, 128, 128], P(None, 'band', 'grid')
- sigma_imag: float32 [2, 8, 128, 128, 128], P(None, 'band', 'grid')
The draws below stay inside these ranges and needn't reach their ends.
All inputs are finite; a program needn't handle non-finite values.
Results may differ from the reference program's by a relative error of at most 0.0003.
Values sent between devices are 32-bit elements; how exact they have to be, the bound alone decides.
A program may use at most 64 MiB of HBM per device.

```python
import math
import jax
import jax.numpy as jnp
from jax import lax

NG = 128
TRIALS = 2
BANDS = 8


def levels(own_key, extent, split, smallest, largest):
    def one(dim, parts):
        steps = jax.random.uniform(jax.random.fold_in(jax.random.fold_in(own_key, 6), dim), (parts,), jnp.float32, smallest / len(split), largest / len(split))
        return jnp.repeat(jnp.exp(steps), extent[dim] // parts).reshape((-1,) + (1,) * (len(extent) - dim - 1))

    gain = one(*split[0])
    for cut in split[1:]:
        gain = gain * one(*cut)
    return gain


def gaussian(own_key, extent, spread, most, cuts=(), kind=jnp.bfloat16):
    drawn = spread * jax.random.normal(own_key, extent, jnp.float32)
    if cuts:
        drawn = drawn * levels(own_key, extent, cuts, -0.22, 0.18)
    return jnp.clip(drawn, -most, most).astype(kind)


def setup_inputs(seed: int = 0) -> dict:
    keys = jax.random.split(jax.random.key(seed), 6)
    return {
        "orbitals": gaussian(keys[0], (BANDS, NG, NG, NG), 0.5, 3.0, ((0, 8), (1, 4))),
        "trial_vectors": gaussian(keys[1], (TRIALS, BANDS, NG, NG, NG), 1.0, 6.0, ((1, 8), (2, 4))),
        "alda_kernel": jnp.clip(-2.0 + 1.5 * jax.random.uniform(keys[2], (NG, NG, NG), jnp.float32) ** levels(keys[2], (NG, NG, NG), ((0, 4),), -0.2, 0.2), -2.0, -0.5),
        "local_potential": jnp.clip(-2.0 + 3.0 * jax.random.uniform(keys[3], (NG, NG, NG), jnp.float32) ** levels(keys[3], (NG, NG, NG), ((0, 4),), -0.2, 0.2), -2.0, 1.0),
        "band_energies": jnp.clip(-1.5 + 1.3 * jax.random.uniform(keys[4], (BANDS,), jnp.float32) ** levels(keys[4], (BANDS,), ((0, 8),), -0.2, 0.2), -1.5, -0.2),
    }


box_length = 30.0


def frequency(length):
    positions = jnp.arange(length, dtype=jnp.int32)
    signed = jnp.where(2 * positions < length, positions, positions - length)
    return signed.astype(jnp.float32)


def coulomb(length):
    signed = frequency(length)
    squared = signed[:, None, None] ** 2 + signed[None, :, None] ** 2 + signed[None, None, :] ** 2
    scaled = (box_length ** 2 / math.pi) / jnp.maximum(squared, 1.0)
    return jnp.where(squared > 0, scaled, 0.0).astype(jnp.float32)


def reference(orbitals, trial_vectors, alda_kernel, local_potential, band_energies):
    length = NG
    kernel = coulomb(length)
    orbital_wide = orbitals.astype(jnp.float32)
    norm_factor = float(length) ** -1.5

    def one_trial(trial_fields):
        density = 2.0 * jnp.sum(trial_fields.astype(jnp.float32) * orbital_wide, axis=0)
        spectrum = jnp.fft.fftn(density) * kernel
        hartree = jnp.real(jnp.fft.ifftn(spectrum)).astype(jnp.float32)
        potential = hartree + alda_kernel * density

        def one_band(member):
            orbital, trial_field, energy = member
            fields = potential * orbital + (local_potential - energy) * trial_field.astype(jnp.float32)
            transformed = jnp.transpose(jnp.fft.fftn(fields), (1, 2, 0)) * norm_factor
            return jnp.real(transformed).astype(jnp.float32), jnp.imag(transformed).astype(jnp.float32)

        return lax.map(one_band, (orbital_wide, trial_fields, band_energies))

    real_parts, imag_parts = lax.map(one_trial, trial_vectors)
    return (real_parts, imag_parts)
```

```python
import functools
import math

import jax
import jax.numpy as jnp
import numpy as np
from jax import lax
from jax.experimental import pallas as pl
from jax.experimental.pallas import tpu as pltpu
from jax.sharding import PartitionSpec as P

box_length = 30.0
f32, bf16 = jnp.float32, jnp.bfloat16
highest = lax.Precision.HIGHEST
vmem_grant = 56 * 1024 * 1024


def tables(length):
    positions = jnp.arange(length, dtype=jnp.int32)
    wrapped = positions[:, None] * positions[None, :] % length
    angles = wrapped.astype(jnp.float32) * (2.0 * math.pi / length)
    return (jnp.cos(angles), jnp.sin(angles))


def contract(pattern, left_operand, right_operand):
    return jnp.einsum(pattern, left_operand, right_operand, precision=highest)


def rotate(pattern, real_part, imag_part, cosine_table, sine_table, orient):
    new_real = contract(pattern, real_part, cosine_table) - orient * contract(
        pattern, imag_part, sine_table
    )
    new_imag = contract(pattern, imag_part, cosine_table) + orient * contract(
        pattern, real_part, sine_table
    )
    return (new_real, new_imag)


def rotate_real(pattern, real_part, cosine_table, sine_table, orient):
    return (
        contract(pattern, real_part, cosine_table),
        orient * contract(pattern, real_part, sine_table),
    )


def frequency(length, offset, extent):
    positions = offset + jnp.arange(extent, dtype=jnp.int32)
    signed = jnp.where(2 * positions < length, positions, positions - length)
    return signed.astype(jnp.float32)


def coulomb_block(first_freq, second_freq, third_freq):
    squared = (
        first_freq[:, None, None] ** 2
        + second_freq[None, :, None] ** 2
        + third_freq[None, None, :] ** 2
    )
    scaled = box_length**2 / math.pi / jnp.maximum(squared, 1.0)
    return jnp.where(squared > 0, scaled, 0.0)


def potential_split(density_share, cosine_table, sine_table, length):
    real_part, imag_part = rotate_real(
        "kxyz,zg->kxgy", density_share, cosine_table, sine_table, -1.0
    )
    arrived = lax.all_to_all(
        jnp.stack((real_part, imag_part)), "band", split_axis=3, concat_axis=4, tiled=True
    )
    real_part, imag_part = rotate(
        "kxzy,yg->kgzx", arrived[0], arrived[1], cosine_table, sine_table, -1.0
    )
    arrived = lax.all_to_all(
        jnp.stack((real_part, imag_part)), "grid", split_axis=2, concat_axis=4, tiled=True
    )
    real_part, imag_part = rotate(
        "kyzx,xg->kyzg", arrived[0], arrived[1], cosine_table, sine_table, -1.0
    )
    rows_here = real_part.shape[1]
    planes_here = real_part.shape[2]
    kernel = coulomb_block(
        frequency(length, lax.axis_index("grid") * rows_here, rows_here),
        frequency(length, lax.axis_index("band") * planes_here, planes_here),
        frequency(length, 0, length),
    )
    real_part = real_part * kernel[None]
    imag_part = imag_part * kernel[None]
    real_part, imag_part = rotate(
        "kyzg,gx->kyzx", real_part, imag_part, cosine_table, sine_table, 1.0
    )
    arrived = lax.all_to_all(
        jnp.stack((real_part, imag_part)), "grid", split_axis=4, concat_axis=2, tiled=True
    )
    real_part, imag_part = rotate(
        "kgzx,gy->kxzy", arrived[0], arrived[1], cosine_table, sine_table, 1.0
    )
    arrived = lax.all_to_all(
        jnp.stack((real_part, imag_part)), "band", split_axis=4, concat_axis=3, tiled=True
    )
    restored = contract("kxgy,gz->kxyz", arrived[0], cosine_table) - contract(
        "kxgy,gz->kxyz", arrived[1], sine_table
    )
    return restored / float(length**3)


def halves(table):
    table = np.asarray(table, np.float32)
    high = table.astype(bf16)
    low = (table - high.astype(np.float32)).astype(bf16)
    return jnp.asarray(high), jnp.asarray(low)


def waves(length, orient):
    index = np.arange(length)
    angles = (index[:, None] * index[None, :] % length) * (2.0 * np.pi / length)
    return np.cos(angles), orient * np.sin(angles)


def right_block(length, orient):
    cosine, sine = waves(length, orient)
    return np.block([[cosine, sine], [-sine, cosine]])


def split(value):
    high = value.astype(bf16)
    return high, (value - high.astype(f32)).astype(bf16)


def mm(left, right):
    return jnp.dot(left, right, preferred_element_type=f32)


def times(value, high, low):
    value_high, value_low = split(value)
    return mm(value_high, high) + (mm(value_low, high) + mm(value_high, low))


def table_times(high, low, value):
    value_high, value_low = split(value)
    return mm(high, value_high) + (mm(high, value_low) + mm(low, value_high))


def plane_forward(length, share, d_ref, zh, zl, yh, yl, out_ref):
    for x in range(share):
        pair = jnp.concatenate([d_ref[x, 0], d_ref[x, 1]], axis=1)
        spec = times(pair, zh[...], zl[...])
        spec = jnp.concatenate([spec[:, :length], spec[:, length:]], axis=0)
        spec = table_times(yh[...], yl[...], spec)
        for part in range(2):
            out_ref[pl.ds(part * share + x, length, stride=2 * share), :] = spec[
                part * length : (part + 1) * length
            ]


def column_filter(length, bs, v_ref, k_ref, fh, fl, ih, il, out_ref):
    if bs == 1:
        values = v_ref[...]
    else:
        values = jnp.concatenate(
            [v_ref[:, b].reshape(2 * length, length) for b in range(bs)], axis=1
        )
    spec = table_times(fh[...], fl[...], values)
    kern = k_ref[...]
    spec = jnp.concatenate([spec[:length] * kern, spec[length:] * kern], axis=0)
    back = table_times(ih[...], il[...], spec)
    if bs == 1:
        out_ref[...] = back
    else:
        for b in range(bs):
            out_ref[:, b] = back[:, b * length : (b + 1) * length].reshape(
                out_ref.shape[0], out_ref.shape[2], length
            )


def plane_backward(length, share, v_ref, d_ref, a_ref, yh, yl, zh, zl, out_ref):
    for x in range(share):
        spec = jnp.concatenate(
            [
                v_ref[pl.ds(part * share + x, length, stride=2 * share), :]
                for part in range(2)
            ],
            axis=0,
        )
        spec = table_times(yh[...], yl[...], spec)
        spec = jnp.concatenate([spec[:length], spec[length:]], axis=1)
        spec = times(spec, zh[...], zl[...])
        for k in range(2):
            out_ref[x, k] = (
                spec[:, k * length : (k + 1) * length] + a_ref[x] * d_ref[x, k]
            )


def field_forward(length, rows, groups, e_ref, p_ref, o_ref, t_ref, l_ref, zh, zl, yh, yl, out_ref):
    width = length // groups
    energy = e_ref[0]
    fields = p_ref[...] * o_ref[...].astype(f32) + (l_ref[...] - energy) * t_ref[
        ...
    ].astype(f32)
    spec = times(fields.reshape(rows * length, length), zh[...], zl[...])
    for x in range(0, rows, 2):
        pair = jnp.concatenate(
            [
                jnp.concatenate(
                    [
                        spec[i * length : (i + 1) * length, :length],
                        spec[i * length : (i + 1) * length, length:],
                    ],
                    axis=0,
                )
                for i in (x, x + 1)
            ],
            axis=1,
        )
        pair = table_times(yh[...], yl[...], pair)
        for i in range(2):
            for part in range(2):
                for g in range(groups):
                    start = part * length + g * width
                    out_ref[g, 0, part, pl.ds(x + i, width, stride=rows), :] = pair[
                        start : start + width, i * length : (i + 1) * length
                    ]


def field_finish(length, rows, count, v_ref, wh, wl, *refs):
    real_ref, imag_ref = refs[-2:]
    for b in range(count):
        value = v_ref[:, :, :, b * rows : (b + 1) * rows, :].reshape(2 * length, length)
        done = times(value.T, wh[...], wl[...])
        real_ref[b] = done[:, :length]
        imag_ref[b] = done[:, length:]


def whole_spec(count):
    return [pl.BlockSpec(memory_space=pltpu.VMEM)] * count


def cost(flops, size):
    return pl.CostEstimate(flops=flops, bytes_accessed=size, transcendentals=0)


def coulomb(length, second, cells):
    def signed(position):
        return jnp.where(2 * position < length, position, position - length).astype(f32)

    along = signed(jnp.arange(length, dtype=jnp.int32))
    squared = (
        along[:, None, None] ** 2
        + signed(second)[None, :, None] ** 2
        + along[None, None, :] ** 2
    )
    scaled = (box_length**2 / math.pi / cells) / jnp.maximum(squared, 1.0)
    return jnp.where(squared > 0, scaled, 0.0)


def plane_potential(bands, groups, orbital, trial, alda_kernel):
    length, x_here = orbital.shape[1], orbital.shape[0]
    share = x_here // bands
    params = pltpu.CompilerParams(vmem_limit_bytes=vmem_grant)
    forward = right_block(length, -1.0)
    backward = right_block(length, 1.0)
    devices = bands * groups
    bs = length // devices
    unit = 2 * length**3

    partial_value = 2.0 * (trial.astype(f32) * orbital.astype(f32)[None])
    partial_value = partial_value.reshape(2, bands, share * length // 16, 16, length)
    partial_value = partial_value.swapaxes(1, 2).reshape(2, -1, bands * 16, length)
    density = lax.psum_scatter(partial_value, "band", scatter_dimension=2, tiled=True)
    density = density.reshape(2, share, length, length).transpose(1, 0, 2, 3)
    alda_rows = lax.dynamic_slice_in_dim(
        alda_kernel, lax.axis_index("band") * share, share, 0
    )
    here = lax.axis_index("band") * groups + lax.axis_index("grid")
    kern = coulomb(
        length, here * bs + jnp.arange(bs, dtype=jnp.int32), float(length**3)
    ).reshape(length, bs * length)

    index = np.arange(devices * 2 * share).reshape(bands, groups, 2, share)
    band_i, grid_i, part_i, row_i = np.unravel_index(index, index.shape)
    order = (part_i * length + grid_i * x_here + band_i * share + row_i).reshape(-1)
    fwd_right, bwd_right = halves(forward), halves(backward)
    fwd_left, bwd_left = halves(forward.T), halves(backward.T)
    column_fwd = halves(forward.T[:, order])
    column_bwd = halves(backward.T[order, :])

    flat = (length * 2 * share, length)
    sent = pl.pallas_call(
        functools.partial(plane_forward, length, share),
        out_shape=jax.ShapeDtypeStruct(flat, f32),
        in_specs=whole_spec(5),
        out_specs=whole_spec(1)[0],
        compiler_params=params,
        cost_estimate=cost(24 * share * unit, 8 * share * length**2 * 4),
    )(density, *fwd_right, *fwd_left)

    both = ("band", "grid")
    block = (devices, bs * 2 * share, length)
    came = lax.all_to_all(sent.reshape(block), both, 0, 0, tiled=True)
    shape = flat if bs == 1 else (devices, bs, 2 * share, length)
    sent = pl.pallas_call(
        functools.partial(column_filter, length, bs),
        out_shape=jax.ShapeDtypeStruct(shape, f32),
        in_specs=whole_spec(6),
        out_specs=whole_spec(1)[0],
        compiler_params=params,
        cost_estimate=cost(24 * bs * unit, 8 * share * length**2 * 4),
    )(came.reshape(shape), kern, *column_fwd, *column_bwd)
    came = lax.all_to_all(sent.reshape(block), both, 0, 0, tiled=True)
    potential_rows = pl.pallas_call(
        functools.partial(plane_backward, length, share),
        out_shape=jax.ShapeDtypeStruct(density.shape, f32),
        in_specs=whole_spec(7),
        out_specs=whole_spec(1)[0],
        compiler_params=params,
        cost_estimate=cost(24 * share * unit, 8 * share * length**2 * 4),
    )(came.reshape(flat), density, alda_rows, *bwd_left, *bwd_right)
    return lax.all_gather(potential_rows, "band", axis=0, tiled=True)


def pencil_potential(orbital, trial, alda_kernel):
    length = orbital.shape[1]
    cosine_table, sine_table = tables(length)
    partial_value = 2.0 * (trial.astype(f32) * orbital.astype(f32)[None])
    density = lax.psum_scatter(partial_value, "band", scatter_dimension=2, tiled=True)
    count = density.shape[2]
    alda_rows = lax.dynamic_slice_in_dim(
        alda_kernel, lax.axis_index("band") * count, count, 1
    )
    hartree = potential_split(density, cosine_table, sine_table, length)
    potential = lax.all_gather(
        hartree + alda_rows[None] * density, "band", axis=2, tiled=True
    )
    return potential.transpose(1, 0, 2, 3)


def per_device(bands, groups, orbitals, trial_vectors, alda_kernel, local_potential, band_energies):
    length = orbitals.shape[2]
    x_here = orbitals.shape[1]
    orbital, trial = orbitals[0], trial_vectors[:, 0]
    params = pltpu.CompilerParams(vmem_limit_bytes=vmem_grant)
    unit = 2 * length**3
    forward = right_block(length, -1.0)
    fwd_left = halves(forward.T)
    if x_here % bands == 0 and length % (bands * groups) == 0 and trial.shape[0] == 2:
        potential = plane_potential(bands, groups, orbital, trial, alda_kernel)
    else:
        potential = pencil_potential(orbital, trial, alda_kernel)

    rows = 8
    steps = x_here // rows
    width = length // groups
    z_table = halves(forward[:length])
    index = np.arange(2 * length).reshape(groups, steps, 2, rows)
    grid_i, step_i, part_i, row_i = np.unravel_index(index, index.shape)
    order = (part_i * length + grid_i * x_here + step_i * rows + row_i).reshape(-1)
    x_table = halves((forward * float(length) ** -1.5)[order])
    trial_count = trial.shape[0]
    table_spec = lambda a, b: pl.BlockSpec((a, b), lambda i: (0, 0))
    cube = (rows, length, length)
    squeezed = pl.Squeezed()
    came = []
    for k in range(trial_count):
        sent = pl.pallas_call(
            functools.partial(field_forward, length, rows, groups),
            grid=(steps,),
            out_shape=jax.ShapeDtypeStruct((groups, steps, 2, width * rows, length), f32),
            in_specs=[
                pl.BlockSpec(memory_space=pltpu.SMEM),
                pl.BlockSpec((rows, squeezed, length, length), lambda i, k=k: (i, k, 0, 0)),
                pl.BlockSpec(cube, lambda i: (i, 0, 0)),
                pl.BlockSpec((squeezed, *cube), lambda i, k=k: (k, i, 0, 0)),
                pl.BlockSpec(cube, lambda i: (i, 0, 0)),
                table_spec(length, 2 * length),
                table_spec(length, 2 * length),
                table_spec(2 * length, 2 * length),
                table_spec(2 * length, 2 * length),
            ],
            out_specs=pl.BlockSpec(
                (groups, 1, 2, width * rows, length), lambda i: (0, i, 0, 0, 0)
            ),
            compiler_params=params,
            cost_estimate=cost(18 * x_here * unit, 8 * x_here * length**2 * 4),
        )(band_energies, potential, orbital, trial, local_potential, *z_table, *fwd_left)
        came.append(lax.all_to_all(sent, "grid", 0, 0, tiled=True))

    count = 8
    full = jax.ShapeDtypeStruct((trial_count, 1, width, length, length), f32)
    results = ()
    for k in range(trial_count):
        out_spec = pl.BlockSpec(
            (squeezed, squeezed, count, length, length), lambda i, k=k: (k, 0, i, 0, 0)
        )
        results = pl.pallas_call(
            functools.partial(field_finish, length, rows, count),
            grid=(width // count,),
            out_shape=(full, full),
            in_specs=[
                pl.BlockSpec(
                    (groups, steps, 2, count * rows, length), lambda i: (0, 0, 0, i, 0)
                ),
                table_spec(2 * length, 2 * length),
                table_spec(2 * length, 2 * length),
            ]
            + [pl.BlockSpec(memory_space=pl.ANY)] * len(results),
            out_specs=(out_spec, out_spec),
            input_output_aliases={3: 0, 4: 1} if results else {},
            compiler_params=params,
            cost_estimate=cost(12 * width * unit, 16 * x_here * length**2 * 4),
        )(came[k], *x_table, *results)
    return tuple(results)


def solution(mesh):
    placed = (
        P("band", "grid", None, None),
        P(None, "band", "grid", None, None),
        P("grid", None, None),
        P("grid", None, None),
        P("band"),
    )
    out = P(None, "band", "grid", None, None)
    return jax.shard_map(
        functools.partial(per_device, mesh.shape["band"], mesh.shape["grid"]),
        mesh=mesh,
        in_specs=placed,
        out_specs=(out, out),
        check_vma=False,
    )
```

```python
import functools
import math

import jax
import jax.numpy as jnp
import numpy as np
from jax import lax
from jax.experimental import pallas as pl
from jax.experimental.pallas import tpu as pltpu
from jax.sharding import PartitionSpec as P

box_length = 30.0
f32, bf16 = jnp.float32, jnp.bfloat16
highest = lax.Precision.HIGHEST
vmem_grant = 56 * 1024 * 1024


def tables(length):
    positions = jnp.arange(length, dtype=jnp.int32)
    wrapped = positions[:, None] * positions[None, :] % length
    angles = wrapped.astype(jnp.float32) * (2.0 * math.pi / length)
    return (jnp.cos(angles), jnp.sin(angles))


def contract(pattern, left_operand, right_operand):
    return jnp.einsum(pattern, left_operand, right_operand, precision=highest)


def rotate(pattern, real_part, imag_part, cosine_table, sine_table, orient):
    new_real = contract(pattern, real_part, cosine_table) - orient * contract(
        pattern, imag_part, sine_table
    )
    new_imag = contract(pattern, imag_part, cosine_table) + orient * contract(
        pattern, real_part, sine_table
    )
    return (new_real, new_imag)


def rotate_real(pattern, real_part, cosine_table, sine_table, orient):
    return (
        contract(pattern, real_part, cosine_table),
        orient * contract(pattern, real_part, sine_table),
    )


def frequency(length, offset, extent):
    positions = offset + jnp.arange(extent, dtype=jnp.int32)
    signed = jnp.where(2 * positions < length, positions, positions - length)
    return signed.astype(jnp.float32)


def coulomb_block(first_freq, second_freq, third_freq):
    squared = (
        first_freq[:, None, None] ** 2
        + second_freq[None, :, None] ** 2
        + third_freq[None, None, :] ** 2
    )
    scaled = box_length**2 / math.pi / jnp.maximum(squared, 1.0)
    return jnp.where(squared > 0, scaled, 0.0)


def potential_split(density_share, cosine_table, sine_table, length):
    real_part, imag_part = rotate_real(
        "kxyz,zg->kxgy", density_share, cosine_table, sine_table, -1.0
    )
    arrived = lax.all_to_all(
        jnp.stack((real_part, imag_part)), "band", split_axis=3, concat_axis=4, tiled=True
    )
    real_part, imag_part = rotate(
        "kxzy,yg->kgzx", arrived[0], arrived[1], cosine_table, sine_table, -1.0
    )
    arrived = lax.all_to_all(
        jnp.stack((real_part, imag_part)), "grid", split_axis=2, concat_axis=4, tiled=True
    )
    real_part, imag_part = rotate(
        "kyzx,xg->kyzg", arrived[0], arrived[1], cosine_table, sine_table, -1.0
    )
    rows_here = real_part.shape[1]
    planes_here = real_part.shape[2]
    kernel = coulomb_block(
        frequency(length, lax.axis_index("grid") * rows_here, rows_here),
        frequency(length, lax.axis_index("band") * planes_here, planes_here),
        frequency(length, 0, length),
    )
    real_part = real_part * kernel[None]
    imag_part = imag_part * kernel[None]
    real_part, imag_part = rotate(
        "kyzg,gx->kyzx", real_part, imag_part, cosine_table, sine_table, 1.0
    )
    arrived = lax.all_to_all(
        jnp.stack((real_part, imag_part)), "grid", split_axis=4, concat_axis=2, tiled=True
    )
    real_part, imag_part = rotate(
        "kgzx,gy->kxzy", arrived[0], arrived[1], cosine_table, sine_table, 1.0
    )
    arrived = lax.all_to_all(
        jnp.stack((real_part, imag_part)), "band", split_axis=4, concat_axis=3, tiled=True
    )
    restored = contract("kxgy,gz->kxyz", arrived[0], cosine_table) - contract(
        "kxgy,gz->kxyz", arrived[1], sine_table
    )
    return restored / float(length**3)


def halves(table):
    table = np.asarray(table, np.float32)
    high = table.astype(bf16)
    low = (table - high.astype(np.float32)).astype(bf16)
    return jnp.asarray(high), jnp.asarray(low)


def waves(length, orient):
    index = np.arange(length)
    angles = (index[:, None] * index[None, :] % length) * (2.0 * np.pi / length)
    return np.cos(angles), orient * np.sin(angles)


def right_block(length, orient):
    cosine, sine = waves(length, orient)
    return np.block([[cosine, sine], [-sine, cosine]])


def split(value):
    high = value.astype(bf16)
    return high, (value - high.astype(f32)).astype(bf16)


def mm(left, right):
    return jnp.dot(left, right, preferred_element_type=f32)


def times(value, high, low):
    value_high, value_low = split(value)
    return mm(value_high, high) + (mm(value_low, high) + mm(value_high, low))


def table_times(high, low, value):
    value_high, value_low = split(value)
    return mm(high, value_high) + (mm(high, value_low) + mm(low, value_high))


def plane_forward(length, share, d_ref, zh, zl, yh, yl, out_ref):
    for x in range(share):
        pair = jnp.concatenate([d_ref[x, 0], d_ref[x, 1]], axis=1)
        spec = times(pair, zh[...], zl[...])
        spec = jnp.concatenate([spec[:, :length], spec[:, length:]], axis=0)
        spec = table_times(yh[...], yl[...], spec)
        for part in range(2):
            out_ref[pl.ds(part * share + x, length, stride=2 * share), :] = spec[
                part * length : (part + 1) * length
            ]


def column_filter(length, bs, v_ref, k_ref, fh, fl, ih, il, out_ref):
    if bs == 1:
        values = v_ref[...]
    else:
        values = jnp.concatenate(
            [v_ref[:, b].reshape(2 * length, length) for b in range(bs)], axis=1
        )
    spec = table_times(fh[...], fl[...], values)
    kern = k_ref[...]
    spec = jnp.concatenate([spec[:length] * kern, spec[length:] * kern], axis=0)
    back = table_times(ih[...], il[...], spec)
    if bs == 1:
        out_ref[...] = back
    else:
        for b in range(bs):
            out_ref[:, b] = back[:, b * length : (b + 1) * length].reshape(
                out_ref.shape[0], out_ref.shape[2], length
            )


def plane_backward(length, share, v_ref, d_ref, a_ref, yh, yl, zh, zl, out_ref):
    for x in range(share):
        spec = jnp.concatenate(
            [
                v_ref[pl.ds(part * share + x, length, stride=2 * share), :]
                for part in range(2)
            ],
            axis=0,
        )
        spec = table_times(yh[...], yl[...], spec)
        spec = jnp.concatenate([spec[:length], spec[length:]], axis=1)
        spec = times(spec, zh[...], zl[...])
        for k in range(2):
            out_ref[k, x] = (
                spec[:, k * length : (k + 1) * length] + a_ref[x] * d_ref[x, k]
            )


def field_forward(length, rows, groups, e_ref, p_ref, o_ref, t_ref, l_ref, zh, zl, yh, yl, out_ref):
    width = length // groups
    energy = e_ref[0]
    fields = p_ref[...] * o_ref[...].astype(f32) + (l_ref[...] - energy) * t_ref[
        ...
    ].astype(f32)
    spec = times(fields.reshape(rows * length, length), zh[...], zl[...])
    for x in range(0, rows, 2):
        pair = jnp.concatenate(
            [
                jnp.concatenate(
                    [
                        spec[i * length : (i + 1) * length, :length],
                        spec[i * length : (i + 1) * length, length:],
                    ],
                    axis=0,
                )
                for i in (x, x + 1)
            ],
            axis=1,
        )
        pair = table_times(yh[...], yl[...], pair)
        for i in range(2):
            for part in range(2):
                for g in range(groups):
                    start = part * length + g * width
                    out_ref[g, 0, part, pl.ds(x + i, width, stride=rows), :] = pair[
                        start : start + width, i * length : (i + 1) * length
                    ]


def field_finish(length, rows, count, v_ref, wh, wl, *refs):
    real_ref, imag_ref = refs[-2:]
    for b in range(count):
        value = v_ref[:, :, :, b * rows : (b + 1) * rows, :].reshape(2 * length, length)
        done = times(value.T, wh[...], wl[...])
        real_ref[b] = done[:, :length]
        imag_ref[b] = done[:, length:]


def whole_spec(count):
    return [pl.BlockSpec(memory_space=pltpu.VMEM)] * count


def cost(flops, size):
    return pl.CostEstimate(flops=flops, bytes_accessed=size, transcendentals=0)


def coulomb(length, second, cells):
    def signed(position):
        return jnp.where(2 * position < length, position, position - length).astype(f32)

    along = signed(jnp.arange(length, dtype=jnp.int32))
    squared = (
        along[:, None, None] ** 2
        + signed(second)[None, :, None] ** 2
        + along[None, None, :] ** 2
    )
    scaled = (box_length**2 / math.pi / cells) / jnp.maximum(squared, 1.0)
    return jnp.where(squared > 0, scaled, 0.0)


def peer(band):
    return {"device_id": {"band": band}, "device_id_type": pl.DeviceIdType.MESH}


def greet(bands):
    barrier = pltpu.get_barrier_semaphore()
    for band in bands:
        pl.semaphore_signal(barrier, inc=1, **peer(band))
    pl.semaphore_wait(barrier, len(bands))


def remote(source, target, sends, receives, slot, band):
    return pltpu.make_async_remote_copy(
        src_ref=source,
        dst_ref=target,
        send_sem=sends.at[slot],
        recv_sem=receives.at[slot],
        **peer(band),
    )


def around(line, here, y):
    near = [2 * here + 1 - y]
    near += [2 * (here + 1) + y] if here + 1 < line else []
    near += [2 * (here - 1) + y] if here > 0 else []
    return near


def reduce_planes(line, share, o_ref, t_ref, out_ref, part, across, up, down, *sems):
    y_send, y_recv, up_send, up_recv, down_send, down_recv = sems
    me = lax.axis_index("band")
    y = lax.rem(me, 2)
    count = share * 2

    @pl.loop(0, 2 * line * share)
    def _(x):
        wide = 2.0 * o_ref[x].astype(f32)
        for k in range(2):
            part[x // share, lax.rem(x, share) * 2 + k] = wide * t_ref[k, x].astype(f32)

    def role(here):
        greet(around(line, here, y))
        order = sorted(range(line), key=lambda j: (-abs(j - here), j < here))
        copies = []
        for j in order:
            copy = remote(
                part.at[2 * j + 1 - y], across.at[j], y_send, y_recv, j, 2 * here + 1 - y
            )
            copy.start()
            copies.append(copy)
        arrived = list(copies)
        for j, copy in zip(order, arrived):
            copy.wait_recv()
            others = [across]
            if j >= here and here > 0:
                remote(part.at[0], up.at[j], up_send, up_recv, j, 2 * here + 1 - y).wait_recv()
                others.append(up)
            if j <= here and here + 1 < line:
                remote(part.at[0], down.at[j], down_send, down_recv, j, 2 * here + 1 - y).wait_recv()
                others.append(down)
            mine = 2 * j + y

            @pl.loop(0, count)
            def _(i):
                total = part[mine, i]
                for other in others:
                    total = total + other[j, i]
                if j == here:
                    out_ref[i] = total
                else:
                    part[mine, i] = total

            if j > here:
                copy = remote(part.at[mine], up.at[j], up_send, up_recv, j, 2 * here + 2 + y)
            elif j < here:
                copy = remote(
                    part.at[mine], down.at[j], down_send, down_recv, j, 2 * here - 2 + y
                )
            if j != here:
                copy.start()
                copies.append(copy)
        for copy in copies:
            copy.wait_send()

    for here in range(line):
        pl.when(me // 2 == here)(functools.partial(role, here))


def gather_planes(line, trial, p_ref, out_ref, held, *sems):
    y_send, y_recv, up_send, up_recv, down_send, down_recv, out_sem = sems
    me = lax.axis_index("band")
    y = lax.rem(me, 2)

    def role(here):
        greet(around(line, here, y))
        copies, outs = [], []

        def keep(source, band, slot):
            copy = pltpu.make_async_copy(source, out_ref.at[band], out_sem.at[slot])
            copy.start()
            outs.append(copy)

        def spread(source, j, upward, downward):
            band = 2 * j + y
            if upward and here + 1 < line:
                copies.append(
                    remote(source, held.at[band], up_send, up_recv, j, 2 * here + 2 + y)
                )
                copies[-1].start()
            if downward and here > 0:
                copies.append(
                    remote(source, held.at[band], down_send, down_recv, j, 2 * here - 2 + y)
                )
                copies[-1].start()
            copies.append(
                remote(source, held.at[band], y_send, y_recv, j, 2 * here + 1 - y)
            )
            copies[-1].start()
            keep(source, band, 2 * j)

        spread(p_ref.at[trial], here, True, True)
        order = [here]
        for far in range(1, line):
            for j, sends, receives in (
                (here - far, up_send, up_recv),
                (here + far, down_send, down_recv),
            ):
                if 0 <= j < line:
                    block = held.at[2 * j + y]
                    remote(block, block, sends, receives, j, 2 * here + 1 - y).wait_recv()
                    spread(block, j, j < here, j > here)
                    order.append(j)
        for j in order:
            block = held.at[2 * j + 1 - y]
            remote(block, block, y_send, y_recv, j, 2 * here + 1 - y).wait_recv()
            keep(block, 2 * j + 1 - y, 2 * j + 1)
        for copy in copies:
            copy.wait_send()
        for copy in outs:
            copy.wait()

    for here in range(line):
        pl.when(me // 2 == here)(functools.partial(role, here))


def reduced(bands, orbital, trial):
    length, x_here = orbital.shape[1], orbital.shape[0]
    share, line = x_here // bands, bands // 2
    block = (share * 2, length, length)
    dma = pltpu.SemaphoreType.DMA((line,))
    out = pl.pallas_call(
        functools.partial(reduce_planes, line, share),
        out_shape=jax.ShapeDtypeStruct(block, f32),
        in_specs=whole_spec(2),
        out_specs=whole_spec(1)[0],
        scratch_shapes=[pltpu.VMEM((bands, *block), f32)]
        + [pltpu.VMEM((line, *block), f32)] * 3
        + [dma] * 6,
        compiler_params=pltpu.CompilerParams(
            vmem_limit_bytes=vmem_grant, collective_id=1, has_side_effects=True
        ),
        cost_estimate=cost(share * length**3, 30 * x_here * length**2 * 4),
    )(orbital, trial)
    return out.reshape(share, 2, length, length)


def gathered(bands, trial, rows):
    share, length = rows.shape[1], rows.shape[2]
    line = bands // 2
    dma = pltpu.SemaphoreType.DMA((line,))
    block = (bands, share, length, length)
    out = pl.pallas_call(
        functools.partial(gather_planes, line, trial),
        out_shape=jax.ShapeDtypeStruct(block, f32),
        in_specs=whole_spec(1),
        out_specs=pl.BlockSpec(memory_space=pl.ANY),
        scratch_shapes=[pltpu.VMEM(block, f32)]
        + [dma] * 6
        + [pltpu.SemaphoreType.DMA((bands,))],
        compiler_params=pltpu.CompilerParams(
            vmem_limit_bytes=vmem_grant, collective_id=2 + trial, has_side_effects=True
        ),
        cost_estimate=cost(share * length**3, 30 * bands * share * length**2 * 4),
    )(rows)
    return out.reshape(bands * share, length, length)


def plane_potential(bands, groups, orbital, trial, alda_kernel):
    length, x_here = orbital.shape[1], orbital.shape[0]
    share = x_here // bands
    params = pltpu.CompilerParams(vmem_limit_bytes=vmem_grant)
    forward = right_block(length, -1.0)
    backward = right_block(length, 1.0)
    devices = bands * groups
    bs = length // devices
    unit = 2 * length**3

    density = reduced(bands, orbital, trial)
    alda_rows = lax.dynamic_slice_in_dim(
        alda_kernel, lax.axis_index("band") * share, share, 0
    )
    here = lax.axis_index("band") * groups + lax.axis_index("grid")
    kern = coulomb(
        length, here * bs + jnp.arange(bs, dtype=jnp.int32), float(length**3)
    ).reshape(length, bs * length)

    index = np.arange(devices * 2 * share).reshape(bands, groups, 2, share)
    band_i, grid_i, part_i, row_i = np.unravel_index(index, index.shape)
    order = (part_i * length + grid_i * x_here + band_i * share + row_i).reshape(-1)
    fwd_right, bwd_right = halves(forward), halves(backward)
    fwd_left, bwd_left = halves(forward.T), halves(backward.T)
    column_fwd = halves(forward.T[:, order])
    column_bwd = halves(backward.T[order, :])

    flat = (length * 2 * share, length)
    sent = pl.pallas_call(
        functools.partial(plane_forward, length, share),
        out_shape=jax.ShapeDtypeStruct(flat, f32),
        in_specs=whole_spec(5),
        out_specs=whole_spec(1)[0],
        compiler_params=params,
        cost_estimate=cost(24 * share * unit, 8 * share * length**2 * 4),
    )(density, *fwd_right, *fwd_left)

    both = ("band", "grid")
    block = (devices, bs * 2 * share, length)
    came = lax.all_to_all(sent.reshape(block), both, 0, 0, tiled=True)
    shape = flat if bs == 1 else (devices, bs, 2 * share, length)
    sent = pl.pallas_call(
        functools.partial(column_filter, length, bs),
        out_shape=jax.ShapeDtypeStruct(shape, f32),
        in_specs=whole_spec(6),
        out_specs=whole_spec(1)[0],
        compiler_params=params,
        cost_estimate=cost(24 * bs * unit, 8 * share * length**2 * 4),
    )(came.reshape(shape), kern, *column_fwd, *column_bwd)
    came = lax.all_to_all(sent.reshape(block), both, 0, 0, tiled=True)
    potential_rows = pl.pallas_call(
        functools.partial(plane_backward, length, share),
        out_shape=jax.ShapeDtypeStruct((2, share, length, length), f32),
        in_specs=whole_spec(7),
        out_specs=whole_spec(1)[0],
        compiler_params=params,
        cost_estimate=cost(24 * share * unit, 8 * share * length**2 * 4),
    )(came.reshape(flat), density, alda_rows, *bwd_left, *bwd_right)
    return [gathered(bands, k, potential_rows) for k in range(2)]


def pencil_potential(orbital, trial, alda_kernel):
    length = orbital.shape[1]
    cosine_table, sine_table = tables(length)
    partial_value = 2.0 * (trial.astype(f32) * orbital.astype(f32)[None])
    density = lax.psum_scatter(partial_value, "band", scatter_dimension=2, tiled=True)
    count = density.shape[2]
    alda_rows = lax.dynamic_slice_in_dim(
        alda_kernel, lax.axis_index("band") * count, count, 1
    )
    hartree = potential_split(density, cosine_table, sine_table, length)
    potential = lax.all_gather(
        hartree + alda_rows[None] * density, "band", axis=2, tiled=True
    )
    return [potential[k] for k in range(trial.shape[0])]


def per_device(bands, groups, orbitals, trial_vectors, alda_kernel, local_potential, band_energies):
    length = orbitals.shape[2]
    x_here = orbitals.shape[1]
    orbital, trial = orbitals[0], trial_vectors[:, 0]
    params = pltpu.CompilerParams(vmem_limit_bytes=vmem_grant)
    unit = 2 * length**3
    forward = right_block(length, -1.0)
    fwd_left = halves(forward.T)
    if (
        bands % 2 == 0
        and x_here % bands == 0
        and length % (bands * groups) == 0
        and trial.shape[0] == 2
    ):
        potential = plane_potential(bands, groups, orbital, trial, alda_kernel)
    else:
        potential = pencil_potential(orbital, trial, alda_kernel)

    rows = 8
    steps = x_here // rows
    width = length // groups
    z_table = halves(forward[:length])
    index = np.arange(2 * length).reshape(groups, steps, 2, rows)
    grid_i, step_i, part_i, row_i = np.unravel_index(index, index.shape)
    order = (part_i * length + grid_i * x_here + step_i * rows + row_i).reshape(-1)
    x_table = halves((forward * float(length) ** -1.5)[order])
    trial_count = trial.shape[0]
    table_spec = lambda a, b: pl.BlockSpec((a, b), lambda i: (0, 0))
    cube = (rows, length, length)
    squeezed = pl.Squeezed()
    came = []
    for k in range(trial_count):
        sent = pl.pallas_call(
            functools.partial(field_forward, length, rows, groups),
            grid=(steps,),
            out_shape=jax.ShapeDtypeStruct((groups, steps, 2, width * rows, length), f32),
            in_specs=[
                pl.BlockSpec(memory_space=pltpu.SMEM),
                pl.BlockSpec(cube, lambda i: (i, 0, 0)),
                pl.BlockSpec(cube, lambda i: (i, 0, 0)),
                pl.BlockSpec((squeezed, *cube), lambda i, k=k: (k, i, 0, 0)),
                pl.BlockSpec(cube, lambda i: (i, 0, 0)),
                table_spec(length, 2 * length),
                table_spec(length, 2 * length),
                table_spec(2 * length, 2 * length),
                table_spec(2 * length, 2 * length),
            ],
            out_specs=pl.BlockSpec(
                (groups, 1, 2, width * rows, length), lambda i: (0, i, 0, 0, 0)
            ),
            compiler_params=params,
            cost_estimate=cost(18 * x_here * unit, 8 * x_here * length**2 * 4),
        )(band_energies, potential[k], orbital, trial, local_potential, *z_table, *fwd_left)
        came.append(lax.all_to_all(sent, "grid", 0, 0, tiled=True))

    count = 8
    full = jax.ShapeDtypeStruct((trial_count, 1, width, length, length), f32)
    results = ()
    for k in range(trial_count):
        out_spec = pl.BlockSpec(
            (squeezed, squeezed, count, length, length), lambda i, k=k: (k, 0, i, 0, 0)
        )
        results = pl.pallas_call(
            functools.partial(field_finish, length, rows, count),
            grid=(width // count,),
            out_shape=(full, full),
            in_specs=[
                pl.BlockSpec(
                    (groups, steps, 2, count * rows, length), lambda i: (0, 0, 0, i, 0)
                ),
                table_spec(2 * length, 2 * length),
                table_spec(2 * length, 2 * length),
            ]
            + [pl.BlockSpec(memory_space=pl.ANY)] * len(results),
            out_specs=(out_spec, out_spec),
            input_output_aliases={3: 0, 4: 1} if results else {},
            compiler_params=params,
            cost_estimate=cost(12 * width * unit, 16 * x_here * length**2 * 4),
        )(came[k], *x_table, *results)
    return tuple(results)


def solution(mesh):
    placed = (
        P("band", "grid", None, None),
        P(None, "band", "grid", None, None),
        P("grid", None, None),
        P("grid", None, None),
        P("band"),
    )
    out = P(None, "band", "grid", None, None)
    return jax.shard_map(
        functools.partial(per_device, mesh.shape["band"], mesh.shape["grid"]),
        mesh=mesh,
        in_specs=placed,
        out_specs=(out, out),
        check_vma=False,
    )
```

```python
import functools
import math

import jax
import jax.numpy as jnp
import numpy as np
from jax import lax
from jax.experimental import pallas as pl
from jax.experimental.pallas import tpu as pltpu
from jax.sharding import PartitionSpec as P

box_length = 30.0
f32, bf16 = jnp.float32, jnp.bfloat16
highest = lax.Precision.HIGHEST
vmem_grant = 56 * 1024 * 1024


def tables(length):
    positions = jnp.arange(length, dtype=jnp.int32)
    wrapped = positions[:, None] * positions[None, :] % length
    angles = wrapped.astype(jnp.float32) * (2.0 * math.pi / length)
    return (jnp.cos(angles), jnp.sin(angles))


def contract(pattern, left_operand, right_operand):
    return jnp.einsum(pattern, left_operand, right_operand, precision=highest)


def rotate(pattern, real_part, imag_part, cosine_table, sine_table, orient):
    new_real = contract(pattern, real_part, cosine_table) - orient * contract(
        pattern, imag_part, sine_table
    )
    new_imag = contract(pattern, imag_part, cosine_table) + orient * contract(
        pattern, real_part, sine_table
    )
    return (new_real, new_imag)


def rotate_real(pattern, real_part, cosine_table, sine_table, orient):
    return (
        contract(pattern, real_part, cosine_table),
        orient * contract(pattern, real_part, sine_table),
    )


def frequency(length, offset, extent):
    positions = offset + jnp.arange(extent, dtype=jnp.int32)
    signed = jnp.where(2 * positions < length, positions, positions - length)
    return signed.astype(jnp.float32)


def coulomb_block(first_freq, second_freq, third_freq):
    squared = (
        first_freq[:, None, None] ** 2
        + second_freq[None, :, None] ** 2
        + third_freq[None, None, :] ** 2
    )
    scaled = box_length**2 / math.pi / jnp.maximum(squared, 1.0)
    return jnp.where(squared > 0, scaled, 0.0)


def potential_split(density_share, cosine_table, sine_table, length):
    real_part, imag_part = rotate_real(
        "kxyz,zg->kxgy", density_share, cosine_table, sine_table, -1.0
    )
    arrived = lax.all_to_all(
        jnp.stack((real_part, imag_part)), "band", split_axis=3, concat_axis=4, tiled=True
    )
    real_part, imag_part = rotate(
        "kxzy,yg->kgzx", arrived[0], arrived[1], cosine_table, sine_table, -1.0
    )
    arrived = lax.all_to_all(
        jnp.stack((real_part, imag_part)), "grid", split_axis=2, concat_axis=4, tiled=True
    )
    real_part, imag_part = rotate(
        "kyzx,xg->kyzg", arrived[0], arrived[1], cosine_table, sine_table, -1.0
    )
    rows_here = real_part.shape[1]
    planes_here = real_part.shape[2]
    kernel = coulomb_block(
        frequency(length, lax.axis_index("grid") * rows_here, rows_here),
        frequency(length, lax.axis_index("band") * planes_here, planes_here),
        frequency(length, 0, length),
    )
    real_part = real_part * kernel[None]
    imag_part = imag_part * kernel[None]
    real_part, imag_part = rotate(
        "kyzg,gx->kyzx", real_part, imag_part, cosine_table, sine_table, 1.0
    )
    arrived = lax.all_to_all(
        jnp.stack((real_part, imag_part)), "grid", split_axis=4, concat_axis=2, tiled=True
    )
    real_part, imag_part = rotate(
        "kgzx,gy->kxzy", arrived[0], arrived[1], cosine_table, sine_table, 1.0
    )
    arrived = lax.all_to_all(
        jnp.stack((real_part, imag_part)), "band", split_axis=4, concat_axis=3, tiled=True
    )
    restored = contract("kxgy,gz->kxyz", arrived[0], cosine_table) - contract(
        "kxgy,gz->kxyz", arrived[1], sine_table
    )
    return restored / float(length**3)


def halves(table):
    table = np.asarray(table, np.float32)
    high = table.astype(bf16)
    low = (table - high.astype(np.float32)).astype(bf16)
    return jnp.asarray(high), jnp.asarray(low)


def waves(length, orient):
    index = np.arange(length)
    angles = (index[:, None] * index[None, :] % length) * (2.0 * np.pi / length)
    return np.cos(angles), orient * np.sin(angles)


def right_block(length, orient):
    cosine, sine = waves(length, orient)
    return np.block([[cosine, sine], [-sine, cosine]])


def split(value):
    high = value.astype(bf16)
    return high, (value - high.astype(f32)).astype(bf16)


def mm(left, right):
    return jnp.dot(left, right, preferred_element_type=f32)


def times(value, high, low):
    value_high, value_low = split(value)
    return mm(value_high, high) + (mm(value_low, high) + mm(value_high, low))


def table_times(high, low, value):
    value_high, value_low = split(value)
    return mm(high, value_high) + (mm(high, value_low) + mm(low, value_high))


def plane_forward(length, share, d_ref, zh, zl, yh, yl, out_ref):
    for x in range(share):
        pair = jnp.concatenate([d_ref[x, 0], d_ref[x, 1]], axis=1)
        spec = times(pair, zh[...], zl[...])
        spec = jnp.concatenate([spec[:, :length], spec[:, length:]], axis=0)
        spec = table_times(yh[...], yl[...], spec)
        for part in range(2):
            out_ref[pl.ds(part * share + x, length, stride=2 * share), :] = spec[
                part * length : (part + 1) * length
            ]


def column_filter(length, bs, v_ref, k_ref, fh, fl, ih, il, out_ref):
    if bs == 1:
        values = v_ref[...]
    else:
        values = jnp.concatenate(
            [v_ref[:, b].reshape(2 * length, length) for b in range(bs)], axis=1
        )
    spec = table_times(fh[...], fl[...], values)
    kern = k_ref[...]
    spec = jnp.concatenate([spec[:length] * kern, spec[length:] * kern], axis=0)
    back = table_times(ih[...], il[...], spec)
    if bs == 1:
        out_ref[...] = back
    else:
        for b in range(bs):
            out_ref[:, b] = back[:, b * length : (b + 1) * length].reshape(
                out_ref.shape[0], out_ref.shape[2], length
            )


def plane_backward(length, share, v_ref, d_ref, a_ref, yh, yl, zh, zl, out_ref):
    for x in range(share):
        spec = jnp.concatenate(
            [
                v_ref[pl.ds(part * share + x, length, stride=2 * share), :]
                for part in range(2)
            ],
            axis=0,
        )
        spec = table_times(yh[...], yl[...], spec)
        spec = jnp.concatenate([spec[:length], spec[length:]], axis=1)
        spec = times(spec, zh[...], zl[...])
        for k in range(2):
            out_ref[k, x] = (
                spec[:, k * length : (k + 1) * length] + a_ref[x] * d_ref[x, k]
            )


def field_forward(length, rows, groups, e_ref, p_ref, o_ref, t_ref, l_ref, zh, zl, yh, yl, out_ref):
    width = length // groups
    energy = e_ref[0]
    fields = p_ref[...] * o_ref[...].astype(f32) + (l_ref[...] - energy) * t_ref[
        ...
    ].astype(f32)
    spec = times(fields.reshape(rows * length, length), zh[...], zl[...])
    for x in range(0, rows, 2):
        pair = jnp.concatenate(
            [
                jnp.concatenate(
                    [
                        spec[i * length : (i + 1) * length, :length],
                        spec[i * length : (i + 1) * length, length:],
                    ],
                    axis=0,
                )
                for i in (x, x + 1)
            ],
            axis=1,
        )
        pair = table_times(yh[...], yl[...], pair)
        for i in range(2):
            for part in range(2):
                for g in range(groups):
                    start = part * length + g * width
                    out_ref[g, 0, part, pl.ds(x + i, width, stride=rows), :] = pair[
                        start : start + width, i * length : (i + 1) * length
                    ]


def field_finish(length, rows, count, v_ref, wh, wl, *refs):
    real_ref, imag_ref = refs[-2:]
    for b in range(count):
        value = v_ref[:, :, :, b * rows : (b + 1) * rows, :].reshape(2 * length, length)
        done = times(value.T, wh[...], wl[...])
        real_ref[b] = done[:, :length]
        imag_ref[b] = done[:, length:]


def whole_spec(count):
    return [pl.BlockSpec(memory_space=pltpu.VMEM)] * count


def cost(flops, size):
    return pl.CostEstimate(flops=flops, bytes_accessed=size, transcendentals=0)


def coulomb(length, second, cells):
    def signed(position):
        return jnp.where(2 * position < length, position, position - length).astype(f32)

    along = signed(jnp.arange(length, dtype=jnp.int32))
    squared = (
        along[:, None, None] ** 2
        + signed(second)[None, :, None] ** 2
        + along[None, None, :] ** 2
    )
    scaled = (box_length**2 / math.pi / cells) / jnp.maximum(squared, 1.0)
    return jnp.where(squared > 0, scaled, 0.0)


def peer(band):
    return {"device_id": {"band": band}, "device_id_type": pl.DeviceIdType.MESH}


def greet(bands):
    barrier = pltpu.get_barrier_semaphore()
    for band in bands:
        pl.semaphore_signal(barrier, inc=1, **peer(band))
    pl.semaphore_wait(barrier, len(bands))


def remote(source, target, sends, receives, slot, band):
    return pltpu.make_async_remote_copy(
        src_ref=source,
        dst_ref=target,
        send_sem=sends.at[slot],
        recv_sem=receives.at[slot],
        **peer(band),
    )


def around(line, here, y):
    near = [2 * here + 1 - y]
    near += [2 * (here + 1) + y] if here + 1 < line else []
    near += [2 * (here - 1) + y] if here > 0 else []
    return near


def reduce_planes(line, share, o_ref, t_ref, out_ref, part, across, up, down, *sems):
    y_send, y_recv, up_send, up_recv, down_send, down_recv = sems
    me = lax.axis_index("band")
    y = lax.rem(me, 2)
    count = share * 2

    def product(block):
        @pl.loop(0, share)
        def _(i):
            x = block * share + i
            wide = 2.0 * o_ref[x].astype(f32)
            for k in range(2):
                part[block, 2 * i + k] = wide * t_ref[k, x].astype(f32)

    def role(here):
        order = sorted(range(line), key=lambda j: (-abs(j - here), j < here))
        copies = []
        blocks = [2 * j + 1 - y for j in order] + [2 * j + y for j in order]
        product(blocks[0])
        greet(around(line, here, y))
        for turn, j in enumerate(order):
            product(blocks[turn + 1])
            copy = remote(
                part.at[2 * j + 1 - y], across.at[j], y_send, y_recv, j, 2 * here + 1 - y
            )
            copy.start()
            copies.append(copy)
        for block in blocks[line + 1 :]:
            product(block)
        arrived = list(copies)
        for j, copy in zip(order, arrived):
            copy.wait_recv()
            others = [across]
            if j >= here and here > 0:
                remote(part.at[0], up.at[j], up_send, up_recv, j, 2 * here + 1 - y).wait_recv()
                others.append(up)
            if j <= here and here + 1 < line:
                remote(part.at[0], down.at[j], down_send, down_recv, j, 2 * here + 1 - y).wait_recv()
                others.append(down)
            mine = 2 * j + y

            @pl.loop(0, count)
            def _(i):
                total = part[mine, i]
                for other in others:
                    total = total + other[j, i]
                if j == here:
                    out_ref[i] = total
                else:
                    part[mine, i] = total

            if j > here:
                copy = remote(part.at[mine], up.at[j], up_send, up_recv, j, 2 * here + 2 + y)
            elif j < here:
                copy = remote(
                    part.at[mine], down.at[j], down_send, down_recv, j, 2 * here - 2 + y
                )
            if j != here:
                copy.start()
                copies.append(copy)
        for copy in copies:
            copy.wait_send()

    for here in range(line):
        pl.when(me // 2 == here)(functools.partial(role, here))


def gather_planes(line, trial, p_ref, out_ref, held, *sems):
    y_send, y_recv, up_send, up_recv, down_send, down_recv, out_sem = sems
    me = lax.axis_index("band")
    y = lax.rem(me, 2)

    def role(here):
        greet(around(line, here, y))
        copies, outs = [], []

        def keep(source, band, slot):
            copy = pltpu.make_async_copy(source, out_ref.at[band], out_sem.at[slot])
            copy.start()
            outs.append(copy)

        def spread(source, j, upward, downward):
            band = 2 * j + y
            if upward and here + 1 < line:
                copies.append(
                    remote(source, held.at[band], up_send, up_recv, j, 2 * here + 2 + y)
                )
                copies[-1].start()
            if downward and here > 0:
                copies.append(
                    remote(source, held.at[band], down_send, down_recv, j, 2 * here - 2 + y)
                )
                copies[-1].start()
            copies.append(
                remote(source, held.at[band], y_send, y_recv, j, 2 * here + 1 - y)
            )
            copies[-1].start()
            keep(source, band, 2 * j)

        spread(p_ref.at[trial], here, True, True)
        order = [here]
        for far in range(1, line):
            for j, sends, receives in (
                (here - far, up_send, up_recv),
                (here + far, down_send, down_recv),
            ):
                if 0 <= j < line:
                    block = held.at[2 * j + y]
                    remote(block, block, sends, receives, j, 2 * here + 1 - y).wait_recv()
                    spread(block, j, j < here, j > here)
                    order.append(j)
        for j in order:
            block = held.at[2 * j + 1 - y]
            remote(block, block, y_send, y_recv, j, 2 * here + 1 - y).wait_recv()
            keep(block, 2 * j + 1 - y, 2 * j + 1)
        for copy in copies:
            copy.wait_send()
        for copy in outs:
            copy.wait()

    for here in range(line):
        pl.when(me // 2 == here)(functools.partial(role, here))


def reduced(bands, orbital, trial):
    length, x_here = orbital.shape[1], orbital.shape[0]
    share, line = x_here // bands, bands // 2
    block = (share * 2, length, length)
    dma = pltpu.SemaphoreType.DMA((line,))
    out = pl.pallas_call(
        functools.partial(reduce_planes, line, share),
        out_shape=jax.ShapeDtypeStruct(block, f32),
        in_specs=whole_spec(2),
        out_specs=whole_spec(1)[0],
        scratch_shapes=[pltpu.VMEM((bands, *block), f32)]
        + [pltpu.VMEM((line, *block), f32)] * 3
        + [dma] * 6,
        compiler_params=pltpu.CompilerParams(
            vmem_limit_bytes=vmem_grant, collective_id=1, has_side_effects=True
        ),
        cost_estimate=cost(share * length**3, 30 * x_here * length**2 * 4),
    )(orbital, trial)
    return out.reshape(share, 2, length, length)


def gathered(bands, trial, rows):
    share, length = rows.shape[1], rows.shape[2]
    line = bands // 2
    dma = pltpu.SemaphoreType.DMA((line,))
    block = (bands, share, length, length)
    out = pl.pallas_call(
        functools.partial(gather_planes, line, trial),
        out_shape=jax.ShapeDtypeStruct(block, f32),
        in_specs=whole_spec(1),
        out_specs=pl.BlockSpec(memory_space=pl.ANY),
        scratch_shapes=[pltpu.VMEM(block, f32)]
        + [dma] * 6
        + [pltpu.SemaphoreType.DMA((bands,))],
        compiler_params=pltpu.CompilerParams(
            vmem_limit_bytes=vmem_grant, collective_id=2 + trial, has_side_effects=True
        ),
        cost_estimate=cost(share * length**3, 30 * bands * share * length**2 * 4),
    )(rows)
    return out.reshape(bands * share, length, length)


def plane_potential(bands, groups, orbital, trial, alda_kernel):
    length, x_here = orbital.shape[1], orbital.shape[0]
    share = x_here // bands
    params = pltpu.CompilerParams(vmem_limit_bytes=vmem_grant)
    forward = right_block(length, -1.0)
    backward = right_block(length, 1.0)
    devices = bands * groups
    bs = length // devices
    unit = 2 * length**3

    density = reduced(bands, orbital, trial)
    alda_rows = lax.dynamic_slice_in_dim(
        alda_kernel, lax.axis_index("band") * share, share, 0
    )
    here = lax.axis_index("band") * groups + lax.axis_index("grid")
    kern = coulomb(
        length, here * bs + jnp.arange(bs, dtype=jnp.int32), float(length**3)
    ).reshape(length, bs * length)

    index = np.arange(devices * 2 * share).reshape(bands, groups, 2, share)
    band_i, grid_i, part_i, row_i = np.unravel_index(index, index.shape)
    order = (part_i * length + grid_i * x_here + band_i * share + row_i).reshape(-1)
    fwd_right, bwd_right = halves(forward), halves(backward)
    fwd_left, bwd_left = halves(forward.T), halves(backward.T)
    column_fwd = halves(forward.T[:, order])
    column_bwd = halves(backward.T[order, :])

    flat = (length * 2 * share, length)
    sent = pl.pallas_call(
        functools.partial(plane_forward, length, share),
        out_shape=jax.ShapeDtypeStruct(flat, f32),
        in_specs=whole_spec(5),
        out_specs=whole_spec(1)[0],
        compiler_params=params,
        cost_estimate=cost(24 * share * unit, 8 * share * length**2 * 4),
    )(density, *fwd_right, *fwd_left)

    both = ("band", "grid")
    block = (devices, bs * 2 * share, length)
    came = lax.all_to_all(sent.reshape(block), both, 0, 0, tiled=True)
    shape = flat if bs == 1 else (devices, bs, 2 * share, length)
    sent = pl.pallas_call(
        functools.partial(column_filter, length, bs),
        out_shape=jax.ShapeDtypeStruct(shape, f32),
        in_specs=whole_spec(6),
        out_specs=whole_spec(1)[0],
        compiler_params=params,
        cost_estimate=cost(24 * bs * unit, 8 * share * length**2 * 4),
    )(came.reshape(shape), kern, *column_fwd, *column_bwd)
    came = lax.all_to_all(sent.reshape(block), both, 0, 0, tiled=True)
    potential_rows = pl.pallas_call(
        functools.partial(plane_backward, length, share),
        out_shape=jax.ShapeDtypeStruct((2, share, length, length), f32),
        in_specs=whole_spec(7),
        out_specs=whole_spec(1)[0],
        compiler_params=params,
        cost_estimate=cost(24 * share * unit, 8 * share * length**2 * 4),
    )(came.reshape(flat), density, alda_rows, *bwd_left, *bwd_right)
    return [gathered(bands, k, potential_rows) for k in range(2)]


def pencil_potential(orbital, trial, alda_kernel):
    length = orbital.shape[1]
    cosine_table, sine_table = tables(length)
    partial_value = 2.0 * (trial.astype(f32) * orbital.astype(f32)[None])
    density = lax.psum_scatter(partial_value, "band", scatter_dimension=2, tiled=True)
    count = density.shape[2]
    alda_rows = lax.dynamic_slice_in_dim(
        alda_kernel, lax.axis_index("band") * count, count, 1
    )
    hartree = potential_split(density, cosine_table, sine_table, length)
    potential = lax.all_gather(
        hartree + alda_rows[None] * density, "band", axis=2, tiled=True
    )
    return [potential[k] for k in range(trial.shape[0])]


def per_device(bands, groups, orbitals, trial_vectors, alda_kernel, local_potential, band_energies):
    length = orbitals.shape[2]
    x_here = orbitals.shape[1]
    orbital, trial = orbitals[0], trial_vectors[:, 0]
    params = pltpu.CompilerParams(vmem_limit_bytes=vmem_grant)
    unit = 2 * length**3
    forward = right_block(length, -1.0)
    fwd_left = halves(forward.T)
    if (
        bands % 2 == 0
        and x_here % bands == 0
        and length % (bands * groups) == 0
        and trial.shape[0] == 2
    ):
        potential = plane_potential(bands, groups, orbital, trial, alda_kernel)
    else:
        potential = pencil_potential(orbital, trial, alda_kernel)

    rows = 8
    steps = x_here // rows
    width = length // groups
    z_table = halves(forward[:length])
    index = np.arange(2 * length).reshape(groups, steps, 2, rows)
    grid_i, step_i, part_i, row_i = np.unravel_index(index, index.shape)
    order = (part_i * length + grid_i * x_here + step_i * rows + row_i).reshape(-1)
    x_table = halves((forward * float(length) ** -1.5)[order])
    trial_count = trial.shape[0]
    table_spec = lambda a, b: pl.BlockSpec((a, b), lambda i: (0, 0))
    cube = (rows, length, length)
    squeezed = pl.Squeezed()
    came = []
    for k in range(trial_count):
        sent = pl.pallas_call(
            functools.partial(field_forward, length, rows, groups),
            grid=(steps,),
            out_shape=jax.ShapeDtypeStruct((groups, steps, 2, width * rows, length), f32),
            in_specs=[
                pl.BlockSpec(memory_space=pltpu.SMEM),
                pl.BlockSpec(cube, lambda i: (i, 0, 0)),
                pl.BlockSpec(cube, lambda i: (i, 0, 0)),
                pl.BlockSpec((squeezed, *cube), lambda i, k=k: (k, i, 0, 0)),
                pl.BlockSpec(cube, lambda i: (i, 0, 0)),
                table_spec(length, 2 * length),
                table_spec(length, 2 * length),
                table_spec(2 * length, 2 * length),
                table_spec(2 * length, 2 * length),
            ],
            out_specs=pl.BlockSpec(
                (groups, 1, 2, width * rows, length), lambda i: (0, i, 0, 0, 0)
            ),
            compiler_params=params,
            cost_estimate=cost(18 * x_here * unit, 8 * x_here * length**2 * 4),
        )(band_energies, potential[k], orbital, trial, local_potential, *z_table, *fwd_left)
        came.append(lax.all_to_all(sent, "grid", 0, 0, tiled=True))

    count = 8
    full = jax.ShapeDtypeStruct((trial_count, 1, width, length, length), f32)
    results = ()
    for k in range(trial_count):
        out_spec = pl.BlockSpec(
            (squeezed, squeezed, count, length, length), lambda i, k=k: (k, 0, i, 0, 0)
        )
        results = pl.pallas_call(
            functools.partial(field_finish, length, rows, count),
            grid=(width // count,),
            out_shape=(full, full),
            in_specs=[
                pl.BlockSpec(
                    (groups, steps, 2, count * rows, length), lambda i: (0, 0, 0, i, 0)
                ),
                table_spec(2 * length, 2 * length),
                table_spec(2 * length, 2 * length),
            ]
            + [pl.BlockSpec(memory_space=pl.ANY)] * len(results),
            out_specs=(out_spec, out_spec),
            input_output_aliases={3: 0, 4: 1} if results else {},
            compiler_params=params,
            cost_estimate=cost(12 * width * unit, 16 * x_here * length**2 * 4),
        )(came[k], *x_table, *results)
    return tuple(results)


def solution(mesh):
    placed = (
        P("band", "grid", None, None),
        P(None, "band", "grid", None, None),
        P("grid", None, None),
        P("grid", None, None),
        P("band"),
    )
    out = P(None, "band", "grid", None, None)
    return jax.shard_map(
        functools.partial(per_device, mesh.shape["band"], mesh.shape["grid"]),
        mesh=mesh,
        in_specs=placed,
        out_specs=(out, out),
        check_vma=False,
    )
```
